256 devices in a mesh: rep: 2 (over x_lo), tbl: 128 (over x_hi, y, z, core).
Axes of the slice: x: 4 (x_hi: 2, x_lo: 2; x = x_hi * 2 + x_lo), y: 4, z: 8, core: 2. Of those that a mesh axis runs over, the one named last changes fastest.
Arguments:
- embeddings: bfloat16 [1048576, 256], P('tbl'), may hold values from -6 to 6
- raw_ids: int32 [1024, 128, 60], P('tbl', 'rep'), may hold values from 0 to 16383
- id_weights: bfloat16 [1024, 128, 60], P('tbl', 'rep'), may hold values from 0.25 to 4
- lengths: int32 [1024, 128], P('tbl', 'rep'), may hold values from 1 to 60
- table_slot: int32 [128], replicated, may hold values from 0 to 127, each once
- table_rows: int32 [128], replicated, may hold values from 1 to 8192, 262144 in all
Outputs:
- pooled: float32 [1024, 128, 256], P('tbl', 'rep')
The draws below stay inside these ranges and needn't reach their ends.
Inputs may be any that keep to these rules, and one draw needn't show every extreme that they name: The bag of request q for table k holds its first lengths[q, k] ids. `table_slot`: each slot holds exactly one table. `table_rows`: some table uses all 8192 rows of its slot.
All inputs are finite; a program needn't handle non-finite values.
Results may differ from the reference program's by a relative error of at most 0.0003.
Values sent between devices are 32-bit elements; how exact they have to be, the bound alone decides.
A program may use at most 64 MiB of HBM per device.

```python
import math
import jax
import jax.numpy as jnp
import numpy as np
from jax import lax

D = 256
ROWS_SLOT = 8192
BAG = 60
TABLES = 128
REQUESTS = 1024


def set_ends(array, rng, low, top_value):
    index_at = [jax.random.randint(jax.random.fold_in(rng, axis), (), 0, length) for axis, length in enumerate(array.shape)]
    longest = array.shape.index(max(array.shape))
    next_to = index_at[:longest] + [(index_at[longest] + 1) % array.shape[longest]] + index_at[longest + 1:]
    return array.at[tuple(index_at)].set(low).at[tuple(next_to)].set(top_value)


def shard_levels(own_key, shape, split, least, largest):
    gain = 1.0
    for position, blocks in split:
        heights = jax.random.uniform(jax.random.fold_in(jax.random.fold_in(own_key, 6), position), (blocks,), jnp.float32, least / len(split), largest / len(split))
        gain = gain * jnp.repeat(jnp.exp(heights), shape[position] // blocks).reshape((-1,) + (1,) * (len(shape) - 1 - position))
    return gain


def rank_bounds(count, skew):
    weights = [(1 << 20) // math.isqrt(standing ** skew) + 1 for standing in range(1, count + 1)]
    spread = 1 + sum(weights) // (1 << 30)
    return np.cumsum(np.array([max(1, weight // spread) for weight in weights]))


def ranked(key, dims, amount, slope):
    grid = rank_bounds(amount, slope)
    ticket = jax.random.randint(jax.random.fold_in(key, 1), dims, 0, int(grid[amount - 1]))
    standing = jnp.searchsorted(jnp.asarray(grid, jnp.int32), ticket, side="right")
    return jax.random.permutation(jax.random.fold_in(key, 2), amount)[standing].astype(jnp.int32)


def split_up(number_of, total, bound, slope):
    portions = [(1 << 20) // math.isqrt(rank ** slope) + 1 for rank in range(2, number_of + 1)]
    surplus, given = total - bound - (number_of - 1), [1] * (number_of - 1)
    while surplus > 0:
        movable = [i for i in range(number_of - 1) if given[i] < bound]
        mass, budget = sum([portions[i] for i in movable]), surplus
        for i in movable:
            more = min(bound - given[i], max(1, budget * portions[i] // mass), surplus)
            given[i] = given[i] + more
            surplus = surplus - more
    return np.array([bound] + given)


def uneven_parts(own_key, amount, total, reach, skew):
    if amount == 2:
        one = jax.random.randint(own_key, (), max(1, total - reach), min(reach, total - 1) + 1)
        return jnp.stack([one, total - one])
    sizes = jnp.asarray(split_up(amount, total, reach, skew), jnp.int32)
    pairs = (amount - 1) // 2
    donor, taker = sizes[1:1 + 2 * pairs:2], sizes[2:2 + 2 * pairs:2]
    margin = jnp.minimum(donor - 1, reach - taker)
    passed = jax.random.randint(jax.random.fold_in(own_key, 1), (pairs,), 0, 1 << 20) % (margin + 1)
    sizes = sizes.at[1:1 + 2 * pairs:2].set(donor - passed).at[2:2 + 2 * pairs:2].set(taker + passed)
    return sizes[jax.random.permutation(jax.random.fold_in(own_key, 2), amount)]


def normal_values(key, shape, deviation, limit, cuts=(), kind=jnp.bfloat16):
    entries = jax.random.normal(key, shape, jnp.float32) * deviation
    if len(cuts) > 0:
        entries = shard_levels(key, shape, cuts, -0.22, 0.18) * entries
    return jnp.clip(entries, min=-limit, max=limit).astype(kind)


def setup_inputs(seed: int = 0) -> dict:
    keys = jax.random.split(jax.random.key(seed), 7)
    embeddings = normal_values(keys[0], (TABLES * ROWS_SLOT, D), 1.0, 6.0, ((0, 128),))
    raw_ids = set_ends(ranked(keys[1], (REQUESTS, TABLES, BAG), 16384, 2), jax.random.fold_in(keys[1], 3), 0, 16383).astype(jnp.int32)
    id_weights = jnp.clip(jnp.exp(math.log(4.0) - 2.7725887 * jax.random.uniform(keys[2], (REQUESTS, TABLES, BAG), jnp.float32) ** shard_levels(keys[2], (REQUESTS, TABLES, BAG), ((0, 128), (1, 2)), -0.2, 0.2)), 0.25, 4.0).astype(jnp.bfloat16)
    lengths = set_ends(jax.random.randint(keys[3], (REQUESTS, TABLES), 1, BAG + 1), jax.random.fold_in(keys[3], 1), 1, BAG).astype(jnp.int32)
    table_slot = jax.random.permutation(keys[4], TABLES).astype(jnp.int32)
    table_rows = uneven_parts(keys[5], TABLES, TABLES * ROWS_SLOT // 4, ROWS_SLOT, 2).astype(jnp.int32)
    return dict(embeddings=embeddings, raw_ids=raw_ids, id_weights=id_weights, lengths=lengths, table_slot=table_slot, table_rows=table_rows)


def reference(embeddings, raw_ids, id_weights, lengths, table_slot, table_rows):
    positions = jnp.arange(BAG, dtype=jnp.int32)

    def pool_table(table_index):
        hashed = lax.dynamic_index_in_dim(raw_ids, table_index, 1, keepdims=False)
        weighting = lax.dynamic_index_in_dim(id_weights, table_index, 1, keepdims=False).astype(jnp.float32)
        counts = lax.dynamic_index_in_dim(lengths, table_index, 1, keepdims=False)
        targets = table_slot[table_index] * ROWS_SLOT + hashed % table_rows[table_index]
        picked = embeddings[targets].astype(jnp.float32)
        live_mask = positions[None, :] < counts[:, None]
        scaled = jnp.where(live_mask, weighting, jnp.float32(0.0))
        summed = jnp.sum(scaled[..., None] * picked, axis=1)
        return summed / counts.astype(jnp.float32)[:, None]

    pooled = lax.map(pool_table, jnp.arange(TABLES, dtype=jnp.int32))
    return jnp.transpose(pooled, (1, 0, 2))
```

```python
import functools

import jax
import jax.numpy as jnp
from jax import lax
from jax.experimental import pallas as pl
from jax.experimental.pallas import tpu as pltpu
from jax.sharding import PartitionSpec as P

MESH = pl.DeviceIdType.MESH
F32, BF16, I32 = jnp.float32, jnp.bfloat16, jnp.int32
SLOTS = 128
BAG = 60
ROWS = 8192
LO = 256
HI = ROWS // LO
CHUNKS = 2
PER = 4 // CHUNKS


def dot_nt(a, b):
    return lax.dot_general(a, b, (((1,), (1,)), ((), ())), preferred_element_type=F32)


def split2(x):
    top = x.astype(BF16)
    return top, (x - top.astype(F32)).astype(BF16)


def build_rows(y_ref, ids_ref, wf_ref, len_ref, half):
    for q in range(4):
        req = 4 * half + q
        count = len_ref[pl.ds(req, 1), :]
        for h in range(2):
            n = 32 if h == 0 else BAG - 32
            start = req + 256 * h
            ids = ids_ref[pl.ds(start, n, stride=8), :].astype(F32)
            w = wf_ref[pl.ds(start, n, stride=8), :]
            pos = lax.broadcasted_iota(I32, (n, 64), 0) + 32 * h
            w = jnp.where(pos < count, w, 0.0)
            y_ref[pl.ds((h * 4 + q) * 32, n), :] = jnp.concatenate([ids, w], axis=1)
            if n < 32:
                y_ref[pl.ds((h * 4 + q) * 32 + n, 32 - n), :] = jnp.zeros((32 - n, 128), F32)


def to_slots(slot_of_lane, y_ref):
    row = lax.broadcasted_iota(I32, (256, 128), 0)
    lane = lax.broadcasted_iota(I32, (256, 128), 1)
    slot = jnp.where(row < 128, row, row - 128)
    pick = (slot_of_lane == slot) & ((row < 128) == (lane < 64))
    pick = jnp.where(pick, 1.0, 0.0).astype(BF16)
    top, rest = split2(y_ref[...])
    return dot_nt(pick, top) + dot_nt(pick, rest)


def place(out_ref, held, ch, half):
    for q in range(PER):
        for c in range(2):
            out_ref[4 * half + ch * PER + q, :, pl.ds(128 * c, 128)] = held[ch, :, 2 * q + c, :]


def kernel(
    ts_smem, ts_ref, tr_ref, ids_ref, w_ref, len_ref, emb_ref,
    out_ref,
    wf, y_own, y_send, y_recv, send1, recv1, key, low, wgt, count, table, acc,
    send2, p_send, p_recv, kept,
    emb_sem, rep_s, rep_r, a_s, a_r, b_s, b_r, c_s, c_r,
    *recv2,
):
    me = lax.axis_index("tbl")
    rep = lax.axis_index("rep")
    other = 1 - rep

    barrier = pltpu.get_barrier_semaphore()

    def greet(d, carry):
        peer = lax.rem(me + d, SLOTS)
        pl.semaphore_signal(barrier, inc=1, device_id={"tbl": peer}, device_id_type=MESH)
        return carry

    lax.fori_loop(1, SLOTS, greet, 0)
    pl.semaphore_signal(barrier, inc=1, device_id={"rep": other}, device_id_type=MESH)

    load = pltpu.make_async_copy(emb_ref, table, emb_sem)
    load.start()

    wf[...] = w_ref[...].astype(F32)
    build_rows(y_send, ids_ref, wf, len_ref, other)
    pl.semaphore_wait(barrier, SLOTS)
    swap = pltpu.make_async_remote_copy(
        y_send, y_recv, rep_s, rep_r, device_id={"rep": other}, device_id_type=MESH
    )
    swap.start()
    build_rows(y_own, ids_ref, wf, len_ref, rep)

    lane = lax.broadcasted_iota(I32, (1, 128), 1)
    slots = ts_ref[...]
    rolled = pltpu.roll(slots, 64, 1)
    first = jnp.where(lane < 64, slots, rolled)
    second = jnp.where(lane < 64, rolled, slots)
    mine = jnp.where(rep == 0, first, second)
    theirs = jnp.where(rep == 0, second, first)
    moved = to_slots(mine, y_own)
    swap.wait()
    moved = moved + to_slots(theirs, y_recv)
    for h in range(2):
        for part in range(2):
            send1[:, 2 * part + h, :] = moved[128 * part : 128 * part + 128, 128 * h : 128 * h + 128]

    def out1(d, carry):
        peer = lax.rem(me + d, SLOTS)
        pltpu.make_async_remote_copy(
            send1.at[peer], recv1.at[me], a_s, a_r, device_id={"tbl": peer}, device_id_type=MESH
        ).start()
        return carry

    lax.fori_loop(1, SLOTS, out1, 0)
    recv1[me] = send1[me]
    all1 = pltpu.make_async_remote_copy(
        send1.at[pl.ds(0, SLOTS - 1)], recv1.at[pl.ds(0, SLOTS - 1)], a_s, a_r,
        device_id={"rep": other}, device_id_type=MESH,
    )
    all1.wait_recv()
    all1.wait_send()

    rows = jnp.sum(jnp.where(slots == me, tr_ref[...], 0), axis=1, keepdims=True).astype(F32)
    src = lax.broadcasted_iota(I32, (128, 128), 0)
    col = lax.broadcasted_iota(I32, (128, 128), 1)
    bag = (4 * lax.rem(src, 2) + col // 32).astype(F32)
    for h in range(2):
        ids = recv1[:, h, :]
        times = jnp.floor((ids + 0.5) / rows)
        row = ids - times * rows
        row = jnp.where(row < 0.0, row + rows, row)
        row = jnp.where(row >= rows, row - rows, row)
        top = jnp.floor(row * (1.0 / LO))
        key[h] = top * 8.0 + bag
        low[h] = row - top * LO
        wgt[h] = recv1[:, 2 + h, :]

    line = lax.broadcasted_iota(I32, (256, 128), 0).astype(F32).astype(BF16)

    def spread(ref, h, t):
        x = jnp.broadcast_to(ref[h, pl.ds(t, 1), :], (16, 128)).astype(BF16)
        return jnp.concatenate([x] * 16, axis=0)

    def count_group(g, carry):
        for p in range(4):
            t = pl.multiple_of(8 * g, 8) + 2 * p
            total = None
            for h in range(2):
                left, right = [], []
                for i in range(2):
                    left.append(jnp.where(spread(key, h, t + i) == line, spread(wgt, h, t + i), jnp.bfloat16(0)))
                    right.append(jnp.where(spread(low, h, t + i) == line, jnp.bfloat16(1), jnp.bfloat16(0)))
                part = dot_nt(jnp.concatenate(left, axis=1), jnp.concatenate(right, axis=1))
                total = part if total is None else total + part
            at = pl.multiple_of(32 * g, 8) + 8 * p
            for c in range(2):
                count[c, :, pl.ds(at, 8), :] = total[:, 128 * c : 128 * c + 128].reshape(HI, 8, 128)
        return carry

    lax.fori_loop(0, SLOTS // 8, count_group, 0)
    load.wait()

    for ch in range(CHUNKS):
        for q in range(PER):
            req = ch * PER + q

            def pool(g, carry):
                total = None
                for i in range(8):
                    hi = 8 * g + i
                    x = jnp.concatenate([count[c, hi, pl.ds(req, 128, stride=4), :] for c in range(2)], axis=1)
                    top, rest = split2(x)
                    part = jnp.dot(
                        jnp.concatenate([top, rest], axis=0),
                        table[pl.ds(pl.multiple_of(hi * LO, LO), LO), :],
                        preferred_element_type=F32,
                    )
                    total = part if total is None else total + part

                @pl.when(g == 0)
                def _():
                    acc[...] = total

                @pl.when(g > 0)
                def _():
                    acc[...] += total

                return carry

            lax.fori_loop(0, HI // 8, pool, 0)
            for c in range(2):
                cols = pl.ds(128 * c, 128)
                send2[ch, :, 2 * q + c, :] = acc[pl.ds(0, 128), cols] + acc[pl.ds(128, 128), cols]

        def out2(d, carry):
            peer = lax.rem(me + d, SLOTS)
            pltpu.make_async_remote_copy(
                send2.at[ch, peer], recv2[ch].at[me], b_s.at[ch], b_r.at[ch],
                device_id={"tbl": peer}, device_id_type=MESH,
            ).start()
            return carry

        lax.fori_loop(1, SLOTS, out2, 0)
        recv2[ch][me] = send2[ch, me]

    swaps = []
    for ch in range(CHUNKS):
        all2 = pltpu.make_async_remote_copy(
            send2.at[ch, pl.ds(0, SLOTS - 1)], recv2[ch].at[pl.ds(0, SLOTS - 1)], b_s.at[ch], b_r.at[ch],
            device_id={"rep": other}, device_id_type=MESH,
        )
        all2.wait_recv()

        def give(k, carry):
            p_send[ch, k] = recv2[ch][ts_smem[64 * other + k]]
            return carry

        lax.fori_loop(0, 64, give, 0)
        swap = pltpu.make_async_remote_copy(
            p_send.at[ch], p_recv.at[ch], c_s.at[ch], c_r.at[ch], device_id={"rep": other}, device_id_type=MESH
        )
        swap.start()
        swaps.append(swap)

        def keep(k, carry):
            kept[ch, k] = recv2[ch][ts_smem[64 * rep + k]]
            return carry

        lax.fori_loop(0, 64, keep, 0)
        place(out_ref, kept, ch, rep)
        all2.wait_send()
    for ch in range(CHUNKS):
        swaps[ch].wait()
        place(out_ref, p_recv, ch, other)


def per_device(embeddings, raw_ids, id_weights, lengths, table_slot, table_rows):
    ids = jnp.transpose(raw_ids, (2, 0, 1)).reshape(8 * BAG, 64)
    weights = jnp.transpose(id_weights, (2, 0, 1)).reshape(8 * BAG, 64)
    vmem = pl.BlockSpec(memory_space=pltpu.VMEM)
    dma = pltpu.SemaphoreType.DMA
    sums = pl.pallas_call(
        kernel,
        out_shape=jax.ShapeDtypeStruct((8, 64, 256), F32),
        in_specs=[pl.BlockSpec(memory_space=pltpu.SMEM), vmem, vmem, vmem, vmem, vmem, pl.BlockSpec(memory_space=pl.ANY)],
        out_specs=vmem,
        scratch_shapes=[
            pltpu.VMEM((8 * BAG, 64), F32),
            pltpu.VMEM((256, 128), F32),
            pltpu.VMEM((256, 128), F32),
            pltpu.VMEM((256, 128), F32),
            pltpu.VMEM((SLOTS, 4, 128), F32),
            pltpu.VMEM((SLOTS, 4, 128), F32),
            pltpu.VMEM((2, 128, 128), F32),
            pltpu.VMEM((2, 128, 128), F32),
            pltpu.VMEM((2, 128, 128), F32),
            pltpu.VMEM((2, HI, 512, 128), F32),
            pltpu.VMEM((ROWS, 256), BF16),
            pltpu.VMEM((256, 256), F32),
            pltpu.VMEM((CHUNKS, SLOTS, 2 * PER, 128), F32),
            pltpu.VMEM((CHUNKS, 64, 2 * PER, 128), F32),
            pltpu.VMEM((CHUNKS, 64, 2 * PER, 128), F32),
            pltpu.VMEM((CHUNKS, 64, 2 * PER, 128), F32),
            dma, dma, dma, dma, dma,
            dma((CHUNKS,)), dma((CHUNKS,)), dma((CHUNKS,)), dma((CHUNKS,)),
        ]
        + [pltpu.VMEM((SLOTS, 2 * PER, 128), F32)] * CHUNKS,
        compiler_params=pltpu.CompilerParams(
            collective_id=0, has_side_effects=True, vmem_limit_bytes=61 * 1024 * 1024
        ),
    )(table_slot, table_slot.reshape(1, 128), table_rows.reshape(1, 128), ids, weights, lengths, embeddings)
    return sums / lengths.astype(F32)[..., None]


def solution(mesh):
    in_specs = (
        P("tbl", None),
        P("tbl", "rep", None),
        P("tbl", "rep", None),
        P("tbl", "rep"),
        P(),
        P(),
    )
    return jax.shard_map(
        per_device, mesh=mesh, in_specs=in_specs, out_specs=P("tbl", "rep", None), check_vma=False
    )
```

```python
import functools

import jax
import jax.numpy as jnp
from jax import lax
from jax.experimental import pallas as pl
from jax.experimental.pallas import tpu as pltpu
from jax.sharding import PartitionSpec as P

MESH = pl.DeviceIdType.MESH
F32, BF16, I32 = jnp.float32, jnp.bfloat16, jnp.int32
SLOTS = 128
BAG = 60
ROWS = 8192
LO = 256
HI = ROWS // LO
CHUNKS = ((0, 2), (2, 1), (3, 1))
MEMBERS = 16
GROUPS = SLOTS // MEMBERS
STEP = 8


def dot_nt(a, b):
    return lax.dot_general(a, b, (((1,), (1,)), ((), ())), preferred_element_type=F32)


def split2(x):
    top = x.astype(BF16)
    return top, (x - top.astype(F32)).astype(BF16)


def build_rows(y_ref, ids_ref, wf_ref, len_ref, half):
    for q in range(4):
        req = 4 * half + q
        count = len_ref[pl.ds(req, 1), :]
        for h in range(2):
            n = 32 if h == 0 else BAG - 32
            start = req + 256 * h
            ids = ids_ref[pl.ds(start, n, stride=8), :].astype(F32)
            w = wf_ref[pl.ds(start, n, stride=8), :]
            pos = lax.broadcasted_iota(I32, (n, 64), 0) + 32 * h
            w = jnp.where(pos < count, w, 0.0)
            y_ref[pl.ds((h * 4 + q) * 32, n), :] = jnp.concatenate([ids, w], axis=1)
            if n < 32:
                y_ref[pl.ds((h * 4 + q) * 32 + n, 32 - n), :] = jnp.zeros((32 - n, 128), F32)


def to_slots(slot_of_lane, y_ref):
    row = lax.broadcasted_iota(I32, (256, 128), 0)
    lane = lax.broadcasted_iota(I32, (256, 128), 1)
    slot = jnp.where(row < 128, row, row - 128)
    pick = (slot_of_lane == slot) & ((row < 128) == (lane < 64))
    pick = jnp.where(pick, 1.0, 0.0).astype(BF16)
    top, rest = split2(y_ref[...])
    return dot_nt(pick, top) + dot_nt(pick, rest)


def place(out_ref, held, inverse, half, first):
    for q in range(held.shape[1] // 2):
        req = 4 * half + first + q
        for c in range(2):
            out_ref[req, :, pl.ds(128 * c, 128)] = held[:, 2 * q + c, :] * inverse[req]


def identity(n):
    row = lax.broadcasted_iota(I32, (n, n), 0)
    return jnp.where(row == lax.broadcasted_iota(I32, (n, n), 1), 1.0, 0.0).astype(BF16)


def kernel(
    ts_smem, ts_ref, tr_ref, ids_ref, w_ref, len_ref, emb_ref,
    out_ref,
    wf, y_own, y_send, y_recv, send1, moved, recv1, key, turned, inverse, count, table, acc,
    emb_sem, rep_s, rep_r, a_s, a_r, b_s, b_r, c_s, c_r,
    *buffers,
):
    send2, recv2, p_send, p_recv, kept = (buffers[i :: 5] for i in range(5))
    me = lax.axis_index("tbl")
    rep = lax.axis_index("rep")
    other = 1 - rep
    group = me // MEMBERS

    barrier = pltpu.get_barrier_semaphore()

    def greet(d, carry):
        peer = lax.rem(me + d, SLOTS)
        pl.semaphore_signal(barrier, inc=1, device_id={"tbl": peer}, device_id_type=MESH)
        return carry

    lax.fori_loop(1, SLOTS, greet, 0)
    pl.semaphore_signal(barrier, inc=1, device_id={"rep": other}, device_id_type=MESH)

    load = pltpu.make_async_copy(emb_ref, table, emb_sem)
    load.start()

    wf[...] = w_ref[...].astype(F32)
    build_rows(y_send, ids_ref, wf, len_ref, other)
    build_rows(y_own, ids_ref, wf, len_ref, rep)
    lane = lax.broadcasted_iota(I32, (1, 128), 1)
    slots = ts_ref[...]
    rolled = pltpu.roll(slots, 64, 1)
    first = jnp.where(lane < 64, slots, rolled)
    second = jnp.where(lane < 64, rolled, slots)
    mine = jnp.where(rep == 0, first, second)
    theirs = jnp.where(rep == 0, second, first)
    moved[...] = to_slots(mine, y_own)
    columns = 1.0 / dot_nt(identity(64), len_ref[...].astype(F32).astype(BF16))
    for req in range(8):
        inverse[req] = jnp.broadcast_to(columns[:, req : req + 1], (64, 128))
    rows = jnp.sum(jnp.where(slots == me, tr_ref[...], 0), axis=1, keepdims=True).astype(F32)
    share = 1.0 / rows

    pl.semaphore_wait(barrier, SLOTS)
    swap = pltpu.make_async_remote_copy(
        y_send, y_recv, rep_s, rep_r, device_id={"rep": other}, device_id_type=MESH
    )
    swap.start()
    swap.wait()
    both = moved[...] + to_slots(theirs, y_recv)
    for h in range(2):
        for part in range(2):
            send1[:, 2 * part + h, :] = both[128 * part : 128 * part + 128, 128 * h : 128 * h + 128]

    def out1(d, carry):
        peer = lax.rem(me + d, SLOTS)
        pltpu.make_async_remote_copy(
            send1.at[peer], recv1.at[me], a_s, a_r.at[group], device_id={"tbl": peer}, device_id_type=MESH
        ).start()
        return carry

    lax.fori_loop(1, SLOTS, out1, 0)
    recv1[me] = send1[me]

    bag = (
        4 * lax.rem(lax.broadcasted_iota(I32, (MEMBERS, 4, 128), 0), 2)
        + lax.broadcasted_iota(I32, (MEMBERS, 4, 128), 2) // 32
    ).astype(F32)
    line = lax.broadcasted_iota(I32, (256, 128), 0).astype(F32).astype(BF16)
    along = lax.broadcasted_iota(I32, (128, 256), 1).astype(F32).astype(BF16)
    unit = identity(128)

    def arrived(n, where):
        return pltpu.make_async_remote_copy(
            send1.at[pl.ds(0, n)], recv1.at[pl.ds(0, n)], a_s, a_r.at[where],
            device_id={"rep": other}, device_id_type=MESH,
        )

    def spread(row):
        x = jnp.broadcast_to(row, (16, 128)).astype(BF16)
        return jnp.concatenate([x] * 16, axis=0)

    def count_group(src):
        base = src * MEMBERS
        ids = recv1[pl.ds(base, MEMBERS)]
        row = ids - jnp.floor((ids + 0.5) * share) * rows
        top = jnp.floor(row * (1.0 / LO))
        key[...] = top * 8.0 + bag
        low = (row - top * LO).reshape(4 * MEMBERS, 128)
        turned[...] = dot_nt(unit, low.astype(BF16))
        for p in range(MEMBERS // 2):
            left, right = [], []
            for h in range(2):
                for i in (2 * p, 2 * p + 1):
                    hit = spread(key[i, pl.ds(h, 1), :]) == line
                    left.append(jnp.where(hit, spread(recv1[base + i, pl.ds(2 + h, 1), :]), jnp.bfloat16(0)))
                    at = 4 * i + h
                    column = jnp.broadcast_to(turned[:, at : at + 1], (128, 256)).astype(BF16)
                    right.append(jnp.where(column == along, jnp.bfloat16(1), jnp.bfloat16(0)))
            total = jnp.dot(
                jnp.concatenate(left, axis=1), jnp.concatenate(right, axis=0), preferred_element_type=F32
            )
            at = pl.multiple_of(4 * MEMBERS * src, 8) + 8 * p
            for c in range(2):
                count[c, :, pl.ds(at, 8), :] = total[:, 128 * c : 128 * c + 128].reshape(HI, 8, 128)

    def count_step(d, carry):
        src = lax.rem(group + GROUPS - d, GROUPS)
        arrived(MEMBERS, src).wait_recv()
        count_group(src)
        return carry

    lax.fori_loop(1, GROUPS, count_step, 0)
    arrived(MEMBERS - 1, group).wait_recv()
    count_group(group)
    load.wait()

    for half in range(2):

        def pool(g, carry):
            total = None
            for i in range(STEP):
                hi = STEP * g + i
                stack = []
                for q in (2 * half, 2 * half + 1):
                    x = jnp.concatenate([count[c, hi, pl.ds(q, 128, stride=4), :] for c in range(2)], axis=1)
                    stack += split2(x)
                part = jnp.dot(
                    jnp.concatenate(stack, axis=0),
                    table[pl.ds(pl.multiple_of(hi * LO, LO), LO), :],
                    preferred_element_type=F32,
                )
                total = part if total is None else total + part

            @pl.when(g == 0)
            def _():
                acc[...] = total

            @pl.when(g > 0)
            def _():
                acc[...] += total

            return carry

        lax.fori_loop(0, HI // STEP, pool, 0)
        for ch, (at, size) in enumerate(CHUNKS):
            if at // 2 != half:
                continue
            for q in range(size):
                for c in range(2):
                    cols = pl.ds(128 * c, 128)
                    up = 256 * (at + q - 2 * half)
                    send2[ch][:, 2 * q + c, :] = acc[pl.ds(up, 128), cols] + acc[pl.ds(up + 128, 128), cols]

            def out2(d, carry):
                peer = lax.rem(me + d, SLOTS)
                pltpu.make_async_remote_copy(
                    send2[ch].at[peer], recv2[ch].at[me], b_s.at[ch], b_r.at[ch],
                    device_id={"tbl": peer}, device_id_type=MESH,
                ).start()
                return carry

            lax.fori_loop(1, SLOTS, out2, 0)
            recv2[ch][me] = send2[ch][me]

    arrived(SLOTS - 1, 0).wait_send()
    ends = []
    for ch, (at, size) in enumerate(CHUNKS):
        everyone = pltpu.make_async_remote_copy(
            send2[ch].at[pl.ds(0, SLOTS - 1)], recv2[ch].at[pl.ds(0, SLOTS - 1)], b_s.at[ch], b_r.at[ch],
            device_id={"rep": other}, device_id_type=MESH,
        )
        everyone.wait_recv()

        def give(k, carry):
            p_send[ch][k] = recv2[ch][ts_smem[64 * other + k]]
            return carry

        lax.fori_loop(0, 64, give, 0, unroll=8)
        back = pltpu.make_async_remote_copy(
            p_send[ch], p_recv[ch], c_s.at[ch], c_r.at[ch], device_id={"rep": other}, device_id_type=MESH
        )
        back.start()
        ends.append((everyone, back))

        def keep(k, carry):
            kept[ch][k] = recv2[ch][ts_smem[64 * rep + k]]
            return carry

        lax.fori_loop(0, 64, keep, 0, unroll=8)
        place(out_ref, kept[ch], inverse, rep, at)
    for ch, (at, size) in enumerate(CHUNKS):
        everyone, back = ends[ch]
        back.wait()
        place(out_ref, p_recv[ch], inverse, other, at)
        everyone.wait_send()


def per_device(embeddings, raw_ids, id_weights, lengths, table_slot, table_rows):
    ids = jnp.transpose(raw_ids, (2, 0, 1)).reshape(8 * BAG, 64)
    weights = jnp.transpose(id_weights, (2, 0, 1)).reshape(8 * BAG, 64)
    vmem = pl.BlockSpec(memory_space=pltpu.VMEM)
    dma = pltpu.SemaphoreType.DMA
    return pl.pallas_call(
        kernel,
        out_shape=jax.ShapeDtypeStruct((8, 64, 256), F32),
        in_specs=[pl.BlockSpec(memory_space=pltpu.SMEM), vmem, vmem, vmem, vmem, vmem, pl.BlockSpec(memory_space=pl.ANY)],
        out_specs=vmem,
        scratch_shapes=[
            pltpu.VMEM((8 * BAG, 64), F32),
            pltpu.VMEM((256, 128), F32),
            pltpu.VMEM((256, 128), F32),
            pltpu.VMEM((256, 128), F32),
            pltpu.VMEM((SLOTS, 4, 128), F32),
            pltpu.VMEM((256, 256), F32),
            pltpu.VMEM((SLOTS, 4, 128), F32),
            pltpu.VMEM((MEMBERS, 4, 128), F32),
            pltpu.VMEM((128, 4 * MEMBERS), F32),
            pltpu.VMEM((8, 64, 128), F32),
            pltpu.VMEM((2, HI, 512, 128), F32),
            pltpu.VMEM((ROWS, 256), BF16),
            pltpu.VMEM((512, 256), F32),
            dma, dma, dma, dma, dma((GROUPS,)),
            dma((len(CHUNKS),)), dma((len(CHUNKS),)), dma((len(CHUNKS),)), dma((len(CHUNKS),)),
        ]
        + [
            pltpu.VMEM((n, 2 * size, 128), F32)
            for _, size in CHUNKS
            for n in (SLOTS, SLOTS, 64, 64, 64)
        ],
        compiler_params=pltpu.CompilerParams(
            collective_id=0, has_side_effects=True, vmem_limit_bytes=61 * 1024 * 1024
        ),
    )(table_slot, table_slot.reshape(1, 128), table_rows.reshape(1, 128), ids, weights, lengths, embeddings)


def solution(mesh):
    in_specs = (
        P("tbl", None),
        P("tbl", "rep", None),
        P("tbl", "rep", None),
        P("tbl", "rep"),
        P(),
        P(),
    )
    return jax.shard_map(
        per_device, mesh=mesh, in_specs=in_specs, out_specs=P("tbl", "rep", None), check_vma=False
    )
```

```python
import functools

import jax
import jax.numpy as jnp
from jax import lax
from jax.experimental import pallas as pl
from jax.experimental.pallas import tpu as pltpu
from jax.sharding import PartitionSpec as P

MESH = pl.DeviceIdType.MESH
F32, BF16, I32 = jnp.float32, jnp.bfloat16, jnp.int32
SLOTS = 128
BAG = 60
ROWS = 8192
LO = 256
HI = ROWS // LO
CHUNKS = ((0, 2), (2, 1), (3, 1))
MEMBERS = 16
GROUPS = SLOTS // MEMBERS
STEP = 16


def dot_nt(a, b):
    return lax.dot_general(a, b, (((1,), (1,)), ((), ())), preferred_element_type=F32)


def split2(x):
    top = x.astype(BF16)
    return top, (x - top.astype(F32)).astype(BF16)


def build_rows(y_ref, ids_ref, wf_ref, len_ref, half):
    for q in range(4):
        req = 4 * half + q
        count = len_ref[pl.ds(req, 1), :]
        for h in range(2):
            n = 32 if h == 0 else BAG - 32
            start = req + 256 * h
            ids = ids_ref[pl.ds(start, n, stride=8), :].astype(F32)
            w = wf_ref[pl.ds(start, n, stride=8), :]
            pos = lax.broadcasted_iota(I32, (n, 64), 0) + 32 * h
            w = jnp.where(pos < count, w, 0.0)
            y_ref[pl.ds((h * 4 + q) * 32, n), :] = jnp.concatenate([ids, w], axis=1)
            if n < 32:
                y_ref[pl.ds((h * 4 + q) * 32 + n, 32 - n), :] = jnp.zeros((32 - n, 128), F32)


def to_slots(slot_of_lane, y_ref):
    row = lax.broadcasted_iota(I32, (256, 128), 0)
    lane = lax.broadcasted_iota(I32, (256, 128), 1)
    slot = jnp.where(row < 128, row, row - 128)
    pick = (slot_of_lane == slot) & ((row < 128) == (lane < 64))
    pick = jnp.where(pick, 1.0, 0.0).astype(BF16)
    top, rest = split2(y_ref[...])
    return dot_nt(pick, top) + dot_nt(pick, rest)


def place(out_ref, held, inverse, half, first):
    for q in range(held.shape[1] // 2):
        req = 4 * half + first + q
        for c in range(2):
            out_ref[req, :, pl.ds(128 * c, 128)] = held[:, 2 * q + c, :] * inverse[req]


def by_z(slot):
    return MEMBERS * (slot // 2 % GROUPS) + 2 * (slot // MEMBERS) + slot % 2


def identity(n):
    row = lax.broadcasted_iota(I32, (n, n), 0)
    return jnp.where(row == lax.broadcasted_iota(I32, (n, n), 1), 1.0, 0.0).astype(BF16)


def kernel(
    ts_smem, ts_ref, tr_ref, ids_ref, w_ref, len_ref, emb_ref,
    out_ref,
    wf, y_own, y_send, y_recv, send1, moved, recv1, key, turned, inverse, count, table, acc,
    emb_sem, rep_s, rep_r, a_s, a_r, b_s, b_r, c_s, c_r,
    *buffers,
):
    send2, recv2, p_send, p_recv, kept = (buffers[i :: 5] for i in range(5))
    me = lax.axis_index("tbl")
    rep = lax.axis_index("rep")
    other = 1 - rep
    mesh_z = lax.rem(me // 2, GROUPS)
    in_z = 2 * (me // MEMBERS) + lax.rem(me, 2)
    mine_at = MEMBERS * mesh_z + in_z

    barrier = pltpu.get_barrier_semaphore()

    def greet(d, carry):
        peer = lax.rem(me + d, SLOTS)
        pl.semaphore_signal(barrier, inc=1, device_id={"tbl": peer}, device_id_type=MESH)
        return carry

    lax.fori_loop(1, SLOTS, greet, 0)
    pl.semaphore_signal(barrier, inc=1, device_id={"rep": other}, device_id_type=MESH)

    load = pltpu.make_async_copy(emb_ref, table, emb_sem)
    load.start()

    wf[...] = w_ref[...].astype(F32)
    build_rows(y_send, ids_ref, wf, len_ref, other)
    build_rows(y_own, ids_ref, wf, len_ref, rep)
    lane = lax.broadcasted_iota(I32, (1, 128), 1)
    slots = by_z(ts_ref[...])
    rolled = pltpu.roll(slots, 64, 1)
    first = jnp.where(lane < 64, slots, rolled)
    second = jnp.where(lane < 64, rolled, slots)
    mine = jnp.where(rep == 0, first, second)
    theirs = jnp.where(rep == 0, second, first)
    moved[...] = to_slots(mine, y_own)
    columns = 1.0 / dot_nt(identity(64), len_ref[...].astype(F32).astype(BF16))
    for req in range(8):
        inverse[req] = jnp.broadcast_to(columns[:, req : req + 1], (64, 128))
    rows = jnp.sum(jnp.where(slots == mine_at, tr_ref[...], 0), axis=1, keepdims=True).astype(F32)
    share = 1.0 / rows

    pl.semaphore_wait(barrier, SLOTS)
    swap = pltpu.make_async_remote_copy(
        y_send, y_recv, rep_s, rep_r, device_id={"rep": other}, device_id_type=MESH
    )
    swap.start()
    swap.wait()
    both = moved[...] + to_slots(theirs, y_recv)
    for h in range(2):
        for part in range(2):
            send1[:, 2 * part + h, :] = both[128 * part : 128 * part + 128, 128 * h : 128 * h + 128]

    def near_first(send):
        for far in range(GROUPS // 2 + 1):
            ways = (far,) if far in (0, GROUPS // 2) else (far, GROUPS - far)

            def one(d, carry):
                at = lax.rem(in_z + d, MEMBERS)
                for way in ways:
                    there = lax.rem(mesh_z + way, GROUPS)
                    send(MEMBERS * (at // 2) + 2 * there + lax.rem(at, 2), MEMBERS * there + at)
                return carry

            lax.fori_loop(1 if far == 0 else 0, MEMBERS, one, 0)

    def in_turn(send):
        def one(d, carry):
            peer = lax.rem(me + d, SLOTS)
            send(peer, MEMBERS * lax.rem(peer // 2, GROUPS) + 2 * (peer // MEMBERS) + lax.rem(peer, 2))
            return carry

        lax.fori_loop(1, SLOTS, one, 0)

    def send_ids(peer, at):
        pltpu.make_async_remote_copy(
            send1.at[at], recv1.at[mine_at], a_s, a_r.at[mesh_z], device_id={"tbl": peer}, device_id_type=MESH
        ).start()

    near_first(send_ids)
    recv1[mine_at] = send1[mine_at]

    bag = (
        4 * lax.rem(lax.broadcasted_iota(I32, (MEMBERS, 4, 128), 0), 2)
        + lax.broadcasted_iota(I32, (MEMBERS, 4, 128), 2) // 32
    ).astype(F32)
    line = lax.broadcasted_iota(I32, (256, 128), 0).astype(F32).astype(BF16)
    along = lax.broadcasted_iota(I32, (128, 256), 1).astype(F32).astype(BF16)
    unit = identity(128)

    def arrived(n, where):
        return pltpu.make_async_remote_copy(
            send1.at[pl.ds(0, n)], recv1.at[pl.ds(0, n)], a_s, a_r.at[where],
            device_id={"rep": other}, device_id_type=MESH,
        )

    def spread(row):
        x = jnp.broadcast_to(row, (16, 128)).astype(BF16)
        return jnp.concatenate([x] * 16, axis=0)

    def count_group(src):
        base = src * MEMBERS
        ids = recv1[pl.ds(base, MEMBERS)]
        row = ids - jnp.floor((ids + 0.5) * share) * rows
        top = jnp.floor(row * (1.0 / LO))
        key[...] = top * 8.0 + bag
        low = (row - top * LO).reshape(4 * MEMBERS, 128)
        turned[...] = dot_nt(unit, low.astype(BF16))
        for p in range(MEMBERS // 2):
            left, right = [], []
            for h in range(2):
                for i in (2 * p, 2 * p + 1):
                    hit = spread(key[i, pl.ds(h, 1), :]) == line
                    left.append(jnp.where(hit, spread(recv1[base + i, pl.ds(2 + h, 1), :]), jnp.bfloat16(0)))
                    at = 4 * i + h
                    column = jnp.broadcast_to(turned[:, at : at + 1], (128, 256)).astype(BF16)
                    right.append(jnp.where(column == along, jnp.bfloat16(1), jnp.bfloat16(0)))
            total = jnp.dot(
                jnp.concatenate(left, axis=1), jnp.concatenate(right, axis=0), preferred_element_type=F32
            )
            at = pl.multiple_of(4 * MEMBERS * src, 8) + 8 * p
            for c in range(2):
                count[c, :, pl.ds(at, 8), :] = total[:, 128 * c : 128 * c + 128].reshape(HI, 8, 128)

    def count_step(d, carry):
        near = (d + 1) // 2
        src = lax.rem(mesh_z + jnp.where(lax.rem(d, 2) == 1, near, GROUPS - near), GROUPS)
        arrived(MEMBERS, src).wait_recv()
        count_group(src)
        return carry

    arrived(MEMBERS - 1, mesh_z).wait_recv()
    count_group(mesh_z)
    lax.fori_loop(1, GROUPS, count_step, 0)
    load.wait()

    for half in range(2):

        def pool(g, carry):
            total = None
            for i in range(STEP):
                hi = STEP * g + i
                stack = []
                for q in (2 * half, 2 * half + 1):
                    x = jnp.concatenate([count[c, hi, pl.ds(q, 128, stride=4), :] for c in range(2)], axis=1)
                    stack += split2(x)
                part = jnp.dot(
                    jnp.concatenate(stack, axis=0),
                    table[pl.ds(pl.multiple_of(hi * LO, LO), LO), :],
                    preferred_element_type=F32,
                )
                total = part if total is None else total + part

            @pl.when(g == 0)
            def _():
                acc[...] = total

            @pl.when(g > 0)
            def _():
                acc[...] += total

            return carry

        lax.fori_loop(0, HI // STEP, pool, 0)
        for ch, (at, size) in enumerate(CHUNKS):
            if at // 2 != half:
                continue
            for q in range(size):
                for c in range(2):
                    cols = pl.ds(128 * c, 128)
                    up = 256 * (at + q - 2 * half)
                    send2[ch][:, 2 * q + c, :] = acc[pl.ds(up, 128), cols] + acc[pl.ds(up + 128, 128), cols]

            def send_sums(peer, at):
                pltpu.make_async_remote_copy(
                    send2[ch].at[at], recv2[ch].at[me], b_s.at[ch], b_r.at[ch],
                    device_id={"tbl": peer}, device_id_type=MESH,
                ).start()

            in_turn(send_sums)
            recv2[ch][me] = send2[ch][mine_at]

    arrived(SLOTS - 1, 0).wait_send()
    ends = []
    for ch, (at, size) in enumerate(CHUNKS):
        everyone = pltpu.make_async_remote_copy(
            send2[ch].at[pl.ds(0, SLOTS - 1)], recv2[ch].at[pl.ds(0, SLOTS - 1)], b_s.at[ch], b_r.at[ch],
            device_id={"rep": other}, device_id_type=MESH,
        )
        everyone.wait_recv()

        def give(k, carry):
            p_send[ch][k] = recv2[ch][ts_smem[64 * other + k]]
            return carry

        lax.fori_loop(0, 64, give, 0, unroll=8)
        back = pltpu.make_async_remote_copy(
            p_send[ch], p_recv[ch], c_s.at[ch], c_r.at[ch], device_id={"rep": other}, device_id_type=MESH
        )
        back.start()
        ends.append((everyone, back))

        def keep(k, carry):
            kept[ch][k] = recv2[ch][ts_smem[64 * rep + k]]
            return carry

        lax.fori_loop(0, 64, keep, 0, unroll=8)
        place(out_ref, kept[ch], inverse, rep, at)
    for ch, (at, size) in enumerate(CHUNKS):
        everyone, back = ends[ch]
        back.wait()
        place(out_ref, p_recv[ch], inverse, other, at)
        everyone.wait_send()


def per_device(embeddings, raw_ids, id_weights, lengths, table_slot, table_rows):
    ids = jnp.transpose(raw_ids, (2, 0, 1)).reshape(8 * BAG, 64)
    weights = jnp.transpose(id_weights, (2, 0, 1)).reshape(8 * BAG, 64)
    vmem = pl.BlockSpec(memory_space=pltpu.VMEM)
    dma = pltpu.SemaphoreType.DMA
    return pl.pallas_call(
        kernel,
        out_shape=jax.ShapeDtypeStruct((8, 64, 256), F32),
        in_specs=[pl.BlockSpec(memory_space=pltpu.SMEM), vmem, vmem, vmem, vmem, vmem, pl.BlockSpec(memory_space=pl.ANY)],
        out_specs=vmem,
        scratch_shapes=[
            pltpu.VMEM((8 * BAG, 64), F32),
            pltpu.VMEM((256, 128), F32),
            pltpu.VMEM((256, 128), F32),
            pltpu.VMEM((256, 128), F32),
            pltpu.VMEM((SLOTS, 4, 128), F32),
            pltpu.VMEM((256, 256), F32),
            pltpu.VMEM((SLOTS, 4, 128), F32),
            pltpu.VMEM((MEMBERS, 4, 128), F32),
            pltpu.VMEM((128, 4 * MEMBERS), F32),
            pltpu.VMEM((8, 64, 128), F32),
            pltpu.VMEM((2, HI, 512, 128), F32),
            pltpu.VMEM((ROWS, 256), BF16),
            pltpu.VMEM((512, 256), F32),
            dma, dma, dma, dma, dma((GROUPS,)),
            dma((len(CHUNKS),)), dma((len(CHUNKS),)), dma((len(CHUNKS),)), dma((len(CHUNKS),)),
        ]
        + [
            pltpu.VMEM((n, 2 * size, 128), F32)
            for _, size in CHUNKS
            for n in (SLOTS, SLOTS, 64, 64, 64)
        ],
        compiler_params=pltpu.CompilerParams(
            collective_id=0, has_side_effects=True, vmem_limit_bytes=61 * 1024 * 1024
        ),
    )(table_slot, table_slot.reshape(1, 128), table_rows.reshape(1, 128), ids, weights, lengths, embeddings)


def solution(mesh):
    in_specs = (
        P("tbl", None),
        P("tbl", "rep", None),
        P("tbl", "rep", None),
        P("tbl", "rep"),
        P(),
        P(),
    )
    return jax.shard_map(
        per_device, mesh=mesh, in_specs=in_specs, out_specs=P("tbl", "rep", None), check_vma=False
    )
```

```python
import functools

import jax
import jax.numpy as jnp
from jax import lax
from jax.experimental import pallas as pl
from jax.experimental.pallas import tpu as pltpu
from jax.sharding import PartitionSpec as P

MESH = pl.DeviceIdType.MESH
F32, BF16, I32 = jnp.float32, jnp.bfloat16, jnp.int32
SLOTS = 128
BAG = 60
ROWS = 8192
LO = 256
HI = ROWS // LO
CHUNKS = ((0, 2), (2, 1), (3, 1))
MEMBERS = 16
GROUPS = SLOTS // MEMBERS
STEP = 16


def dot_nt(a, b):
    return lax.dot_general(a, b, (((1,), (1,)), ((), ())), preferred_element_type=F32)


def split2(x):
    top = x.astype(BF16)
    return top, (x - top.astype(F32)).astype(BF16)


def build_rows(y_ref, ids_ref, wf_ref, len_ref, half):
    for q in range(4):
        req = 4 * half + q
        count = len_ref[pl.ds(req, 1), :]
        for h in range(2):
            n = 32 if h == 0 else BAG - 32
            start = req + 256 * h
            ids = ids_ref[pl.ds(start, n, stride=8), :].astype(F32)
            w = wf_ref[pl.ds(start, n, stride=8), :]
            pos = lax.broadcasted_iota(I32, (n, 64), 0) + 32 * h
            w = jnp.where(pos < count, w, 0.0)
            y_ref[pl.ds((h * 4 + q) * 32, n), :] = jnp.concatenate([ids, w], axis=1)
            if n < 32:
                y_ref[pl.ds((h * 4 + q) * 32 + n, 32 - n), :] = jnp.zeros((32 - n, 128), F32)


def to_slots(slot_of_lane, y_ref):
    row = lax.broadcasted_iota(I32, (256, 128), 0)
    lane = lax.broadcasted_iota(I32, (256, 128), 1)
    slot = jnp.where(row < 128, row, row - 128)
    pick = (slot_of_lane == slot) & ((row < 128) == (lane < 64))
    pick = jnp.where(pick, 1.0, 0.0).astype(BF16)
    top, rest = split2(y_ref[...])
    return dot_nt(pick, top) + dot_nt(pick, rest)


def place(out_ref, held, inverse, half, first):
    for q in range(held.shape[1] // 2):
        req = 4 * half + first + q
        for c in range(2):
            out_ref[req, :, pl.ds(128 * c, 128)] = held[:, 2 * q + c, :] * inverse[req]


def by_z(slot):
    return MEMBERS * (slot // 2 % GROUPS) + 2 * (slot // MEMBERS) + slot % 2


def identity(n):
    row = lax.broadcasted_iota(I32, (n, n), 0)
    return jnp.where(row == lax.broadcasted_iota(I32, (n, n), 1), 1.0, 0.0).astype(BF16)


def kernel(
    ts_smem, ts_hbm, tr_hbm, ids_hbm, w_hbm, len_hbm, emb_ref,
    out_ref,
    wf, y_own, y_send, y_recv, send1, moved, recv1, key, turned, inverse, count, table, acc,
    ts_ref, tr_ref, ids_ref, w_ref, len_ref, in_sem, emb_sem, rep_s, rep_r, a_s, a_r, b_s, b_r, c_s, c_r,
    *buffers,
):
    send2, recv2, p_send, p_recv, kept = (buffers[i :: 5] for i in range(5))
    me = lax.axis_index("tbl")
    rep = lax.axis_index("rep")
    other = 1 - rep
    mesh_z = lax.rem(me // 2, GROUPS)
    in_z = 2 * (me // MEMBERS) + lax.rem(me, 2)
    mine_at = MEMBERS * mesh_z + in_z

    inputs = [
        pltpu.make_async_copy(src, dst, in_sem.at[i])
        for i, (src, dst) in enumerate(
            [(ids_hbm, ids_ref), (w_hbm, w_ref), (len_hbm, len_ref), (ts_hbm, ts_ref), (tr_hbm, tr_ref)]
        )
    ]
    for copy in inputs:
        copy.start()
    barrier = pltpu.get_barrier_semaphore()

    def greet(d, carry):
        peer = lax.rem(me + d, SLOTS)
        pl.semaphore_signal(barrier, inc=1, device_id={"tbl": peer}, device_id_type=MESH)
        return carry

    lax.fori_loop(1, SLOTS, greet, 0)
    pl.semaphore_signal(barrier, inc=1, device_id={"rep": other}, device_id_type=MESH)

    load = pltpu.make_async_copy(emb_ref, table, emb_sem)
    load.start()

    for copy in inputs:
        copy.wait()
    wf[...] = w_ref[...].astype(F32)
    build_rows(y_send, ids_ref, wf, len_ref, other)
    build_rows(y_own, ids_ref, wf, len_ref, rep)
    lane = lax.broadcasted_iota(I32, (1, 128), 1)
    slots = by_z(ts_ref[...])
    rolled = pltpu.roll(slots, 64, 1)
    first = jnp.where(lane < 64, slots, rolled)
    second = jnp.where(lane < 64, rolled, slots)
    mine = jnp.where(rep == 0, first, second)
    theirs = jnp.where(rep == 0, second, first)
    moved[...] = to_slots(mine, y_own)
    columns = 1.0 / dot_nt(identity(64), len_ref[...].astype(F32).astype(BF16))
    for req in range(8):
        inverse[req] = jnp.broadcast_to(columns[:, req : req + 1], (64, 128))
    rows = jnp.sum(jnp.where(slots == mine_at, tr_ref[...], 0), axis=1, keepdims=True).astype(F32)
    share = 1.0 / rows

    pl.semaphore_wait(barrier, SLOTS)
    swap = pltpu.make_async_remote_copy(
        y_send, y_recv, rep_s, rep_r, device_id={"rep": other}, device_id_type=MESH
    )
    swap.start()
    swap.wait()
    both = moved[...] + to_slots(theirs, y_recv)
    for h in range(2):
        for part in range(2):
            send1[:, 2 * part + h, :] = both[128 * part : 128 * part + 128, 128 * h : 128 * h + 128]

    def to_all(send, phases):
        for phase in phases:
            slabs = [(way, lax.rem(mesh_z + way, GROUPS)) for way in phase]

            def row(d, skip):
                at = lax.rem(in_z + d, MEMBERS)
                base = MEMBERS * (at // 2) + lax.rem(at, 2)
                for way, there in slabs:
                    if not (skip and way == 0):
                        send(base + 2 * there, MEMBERS * there + at)

            def one(d, carry):
                row(d, False)
                return carry

            row(0, True)
            lax.fori_loop(1, MEMBERS, one, 0)

    def send_ids(peer, at):
        pltpu.make_async_remote_copy(
            send1.at[at], recv1.at[mine_at], a_s, a_r.at[mesh_z], device_id={"tbl": peer}, device_id_type=MESH
        ).start()

    to_all(send_ids, ((1, 7, 0), (2, 6), (3, 5, 4)))
    recv1[mine_at] = send1[mine_at]

    bag = (
        4 * lax.rem(lax.broadcasted_iota(I32, (MEMBERS, 4, 128), 0), 2)
        + lax.broadcasted_iota(I32, (MEMBERS, 4, 128), 2) // 32
    ).astype(F32)
    line = lax.broadcasted_iota(I32, (256, 128), 0).astype(F32).astype(BF16)
    along = lax.broadcasted_iota(I32, (128, 256), 1).astype(F32).astype(BF16)
    unit = identity(128)

    def arrived(n, where):
        return pltpu.make_async_remote_copy(
            send1.at[pl.ds(0, n)], recv1.at[pl.ds(0, n)], a_s, a_r.at[where],
            device_id={"rep": other}, device_id_type=MESH,
        )

    def spread(row):
        x = jnp.broadcast_to(row, (16, 128)).astype(BF16)
        return jnp.concatenate([x] * 16, axis=0)

    def count_group(src):
        base = src * MEMBERS
        ids = recv1[pl.ds(base, MEMBERS)]
        row = ids - jnp.floor((ids + 0.5) * share) * rows
        top = jnp.floor(row * (1.0 / LO))
        key[...] = top * 8.0 + bag
        low = (row - top * LO).reshape(4 * MEMBERS, 128)
        turned[...] = dot_nt(unit, low.astype(BF16))
        for p in range(MEMBERS // 2):
            left, right = [], []
            for h in range(2):
                for i in (2 * p, 2 * p + 1):
                    hit = spread(key[i, pl.ds(h, 1), :]) == line
                    left.append(jnp.where(hit, spread(recv1[base + i, pl.ds(2 + h, 1), :]), jnp.bfloat16(0)))
                    at = 4 * i + h
                    column = jnp.broadcast_to(turned[:, at : at + 1], (128, 256)).astype(BF16)
                    right.append(jnp.where(column == along, jnp.bfloat16(1), jnp.bfloat16(0)))
            total = jnp.dot(
                jnp.concatenate(left, axis=1), jnp.concatenate(right, axis=0), preferred_element_type=F32
            )
            at = pl.multiple_of(4 * MEMBERS * src, 8) + 8 * p
            for c in range(2):
                count[c, :, pl.ds(at, 8), :] = total[:, 128 * c : 128 * c + 128].reshape(HI, 8, 128)

    def count_step(d, carry):
        near = (d + 1) // 2
        src = lax.rem(mesh_z + jnp.where(lax.rem(d, 2) == 1, near, GROUPS - near), GROUPS)
        arrived(MEMBERS, src).wait_recv()
        count_group(src)
        return carry

    arrived(MEMBERS - 1, mesh_z).wait_recv()
    count_group(mesh_z)
    lax.fori_loop(1, GROUPS, count_step, 0)
    load.wait()

    for half in range(2):

        def pool(g, carry):
            total = None
            for i in range(STEP):
                hi = STEP * g + i
                stack = []
                for q in (2 * half, 2 * half + 1):
                    x = jnp.concatenate([count[c, hi, pl.ds(q, 128, stride=4), :] for c in range(2)], axis=1)
                    stack += split2(x)
                part = jnp.dot(
                    jnp.concatenate(stack, axis=0),
                    table[pl.ds(pl.multiple_of(hi * LO, LO), LO), :],
                    preferred_element_type=F32,
                )
                total = part if total is None else total + part

            @pl.when(g == 0)
            def _():
                acc[...] = total

            @pl.when(g > 0)
            def _():
                acc[...] += total

            return carry

        lax.fori_loop(0, HI // STEP, pool, 0)
        for ch, (at, size) in enumerate(CHUNKS):
            if at // 2 != half:
                continue
            for q in range(size):
                for c in range(2):
                    cols = pl.ds(128 * c, 128)
                    up = 256 * (at + q - 2 * half)
                    send2[ch][:, 2 * q + c, :] = acc[pl.ds(up, 128), cols] + acc[pl.ds(up + 128, 128), cols]

            def send_sums(peer, at):
                pltpu.make_async_remote_copy(
                    send2[ch].at[at], recv2[ch].at[me], b_s.at[ch], b_r.at[ch],
                    device_id={"tbl": peer}, device_id_type=MESH,
                ).start()

            to_all(send_sums, ((4, 1, 7, 2, 6, 3, 5, 0),))
            recv2[ch][me] = send2[ch][mine_at]

    arrived(SLOTS - 1, 0).wait_send()
    ends = []
    for ch, (at, size) in enumerate(CHUNKS):
        everyone = pltpu.make_async_remote_copy(
            send2[ch].at[pl.ds(0, SLOTS - 1)], recv2[ch].at[pl.ds(0, SLOTS - 1)], b_s.at[ch], b_r.at[ch],
            device_id={"rep": other}, device_id_type=MESH,
        )
        everyone.wait_recv()

        def give(k, carry):
            p_send[ch][k] = recv2[ch][ts_smem[64 * other + k]]
            return carry

        lax.fori_loop(0, 64, give, 0, unroll=8)
        back = pltpu.make_async_remote_copy(
            p_send[ch], p_recv[ch], c_s.at[ch], c_r.at[ch], device_id={"rep": other}, device_id_type=MESH
        )
        back.start()
        ends.append((everyone, back))

        def keep(k, carry):
            kept[ch][k] = recv2[ch][ts_smem[64 * rep + k]]
            return carry

        lax.fori_loop(0, 64, keep, 0, unroll=8)
        place(out_ref, kept[ch], inverse, rep, at)
    for ch, (at, size) in enumerate(CHUNKS):
        everyone, back = ends[ch]
        back.wait()
        place(out_ref, p_recv[ch], inverse, other, at)
        everyone.wait_send()


def per_device(embeddings, raw_ids, id_weights, lengths, table_slot, table_rows):
    ids = jnp.transpose(raw_ids, (2, 0, 1)).reshape(8 * BAG, 64)
    weights = jnp.transpose(id_weights, (2, 0, 1)).reshape(8 * BAG, 64)
    vmem = pl.BlockSpec(memory_space=pltpu.VMEM)
    dma = pltpu.SemaphoreType.DMA
    return pl.pallas_call(
        kernel,
        out_shape=jax.ShapeDtypeStruct((8, 64, 256), F32),
        in_specs=[pl.BlockSpec(memory_space=pltpu.SMEM)] + [pl.BlockSpec(memory_space=pltpu.HBM)] * 6,
        out_specs=vmem,
        scratch_shapes=[
            pltpu.VMEM((8 * BAG, 64), F32),
            pltpu.VMEM((256, 128), F32),
            pltpu.VMEM((256, 128), F32),
            pltpu.VMEM((256, 128), F32),
            pltpu.VMEM((SLOTS, 4, 128), F32),
            pltpu.VMEM((256, 256), F32),
            pltpu.VMEM((SLOTS, 4, 128), F32),
            pltpu.VMEM((MEMBERS, 4, 128), F32),
            pltpu.VMEM((128, 4 * MEMBERS), F32),
            pltpu.VMEM((8, 64, 128), F32),
            pltpu.VMEM((2, HI, 512, 128), F32),
            pltpu.VMEM((ROWS, 256), BF16),
            pltpu.VMEM((512, 256), F32),
            pltpu.VMEM((1, 128), I32),
            pltpu.VMEM((1, 128), I32),
            pltpu.VMEM((8 * BAG, 64), I32),
            pltpu.VMEM((8 * BAG, 64), BF16),
            pltpu.VMEM((8, 64), I32),
            dma((5,)),
            dma, dma, dma, dma, dma((GROUPS,)),
            dma((len(CHUNKS),)), dma((len(CHUNKS),)), dma((len(CHUNKS),)), dma((len(CHUNKS),)),
        ]
        + [
            pltpu.VMEM((n, 2 * size, 128), F32)
            for _, size in CHUNKS
            for n in (SLOTS, SLOTS, 64, 64, 64)
        ],
        compiler_params=pltpu.CompilerParams(
            collective_id=0, has_side_effects=True, vmem_limit_bytes=61 * 1024 * 1024
        ),
    )(table_slot, table_slot.reshape(1, 128), table_rows.reshape(1, 128), ids, weights, lengths, embeddings)


def solution(mesh):
    in_specs = (
        P("tbl", None),
        P("tbl", "rep", None),
        P("tbl", "rep", None),
        P("tbl", "rep"),
        P(),
        P(),
    )
    return jax.shard_map(
        per_device, mesh=mesh, in_specs=in_specs, out_specs=P("tbl", "rep", None), check_vma=False
    )
```

```python
import functools

import jax
import jax.numpy as jnp
from jax import lax
from jax.experimental import pallas as pl
from jax.experimental.pallas import tpu as pltpu
from jax.sharding import PartitionSpec as P

MESH = pl.DeviceIdType.MESH
F32, BF16, I32 = jnp.float32, jnp.bfloat16, jnp.int32
SLOTS = 128
BAG = 60
ROWS = 8192
LO = 256
HI = ROWS // LO
CHUNKS = ((0, 1), (1, 1), (2, 1), (3, 1))
BLOCKS = ((0,), (1,), (2,), (3,))
MEMBERS = 16
GROUPS = SLOTS // MEMBERS
STEP = 16


def dot_nt(a, b):
    return lax.dot_general(a, b, (((1,), (1,)), ((), ())), preferred_element_type=F32)


def split2(x):
    top = x.astype(BF16)
    return top, (x - top.astype(F32)).astype(BF16)


def build_rows(y_ref, ids_ref, wf_ref, len_ref, half):
    for q in range(4):
        req = 4 * half + q
        count = len_ref[pl.ds(req, 1), :]
        for h in range(2):
            n = 32 if h == 0 else BAG - 32
            start = req + 256 * h
            ids = ids_ref[pl.ds(start, n, stride=8), :].astype(F32)
            w = wf_ref[pl.ds(start, n, stride=8), :]
            pos = lax.broadcasted_iota(I32, (n, 64), 0) + 32 * h
            w = jnp.where(pos < count, w, 0.0)
            y_ref[pl.ds((h * 4 + q) * 32, n), :] = jnp.concatenate([ids, w], axis=1)
            if n < 32:
                y_ref[pl.ds((h * 4 + q) * 32 + n, 32 - n), :] = jnp.zeros((32 - n, 128), F32)


def to_slots(slot_of_lane, y_ref):
    row = lax.broadcasted_iota(I32, (256, 128), 0)
    lane = lax.broadcasted_iota(I32, (256, 128), 1)
    slot = jnp.where(row < 128, row, row - 128)
    pick = (slot_of_lane == slot) & ((row < 128) == (lane < 64))
    pick = jnp.where(pick, 1.0, 0.0).astype(BF16)
    top, rest = split2(y_ref[...])
    return dot_nt(pick, top) + dot_nt(pick, rest)


def place(out_ref, held, inverse, half, first):
    for q in range(held.shape[1] // 2):
        req = 4 * half + first + q
        for c in range(2):
            out_ref[req, :, pl.ds(128 * c, 128)] = held[:, 2 * q + c, :] * inverse[req]


def by_z(slot):
    return MEMBERS * (slot // 2 % GROUPS) + 2 * (slot // MEMBERS) + slot % 2


def identity(n):
    row = lax.broadcasted_iota(I32, (n, n), 0)
    return jnp.where(row == lax.broadcasted_iota(I32, (n, n), 1), 1.0, 0.0).astype(BF16)


def kernel(
    ts_smem, ts_hbm, tr_hbm, ids_hbm, w_hbm, len_hbm, emb_ref,
    out_ref,
    wf, y_own, y_send, y_recv, send1, moved, recv1, key, turned, inverse, count, table, acc,
    ts_ref, tr_ref, ids_ref, w_ref, len_ref, in_sem, emb_sem, rep_s, rep_r, a_s, a_r, b_s, b_r, c_s, c_r,
    *buffers,
):
    send2, recv2, p_send, p_recv, kept = (buffers[i :: 5] for i in range(5))
    me = lax.axis_index("tbl")
    rep = lax.axis_index("rep")
    other = 1 - rep
    mesh_z = lax.rem(me // 2, GROUPS)
    in_z = 2 * (me // MEMBERS) + lax.rem(me, 2)
    mine_at = MEMBERS * mesh_z + in_z

    inputs = [
        pltpu.make_async_copy(src, dst, in_sem.at[i])
        for i, (src, dst) in enumerate(
            [(ids_hbm, ids_ref), (w_hbm, w_ref), (len_hbm, len_ref), (ts_hbm, ts_ref), (tr_hbm, tr_ref)]
        )
    ]
    for copy in inputs:
        copy.start()
    barrier = pltpu.get_barrier_semaphore()

    def greet(d, carry):
        peer = lax.rem(me + d, SLOTS)
        pl.semaphore_signal(barrier, inc=1, device_id={"tbl": peer}, device_id_type=MESH)
        return carry

    lax.fori_loop(1, SLOTS, greet, 0)
    pl.semaphore_signal(barrier, inc=1, device_id={"rep": other}, device_id_type=MESH)

    load = pltpu.make_async_copy(emb_ref, table, emb_sem)
    load.start()

    for copy in inputs:
        copy.wait()
    wf[...] = w_ref[...].astype(F32)
    build_rows(y_send, ids_ref, wf, len_ref, other)
    build_rows(y_own, ids_ref, wf, len_ref, rep)
    lane = lax.broadcasted_iota(I32, (1, 128), 1)
    slots = by_z(ts_ref[...])
    rolled = pltpu.roll(slots, 64, 1)
    first = jnp.where(lane < 64, slots, rolled)
    second = jnp.where(lane < 64, rolled, slots)
    mine = jnp.where(rep == 0, first, second)
    theirs = jnp.where(rep == 0, second, first)
    moved[...] = to_slots(mine, y_own)
    columns = 1.0 / dot_nt(identity(64), len_ref[...].astype(F32).astype(BF16))
    for req in range(8):
        inverse[req] = jnp.broadcast_to(columns[:, req : req + 1], (64, 128))
    rows = jnp.sum(jnp.where(slots == mine_at, tr_ref[...], 0), axis=1, keepdims=True).astype(F32)
    share = 1.0 / rows

    pl.semaphore_wait(barrier, SLOTS)
    swap = pltpu.make_async_remote_copy(
        y_send, y_recv, rep_s, rep_r, device_id={"rep": other}, device_id_type=MESH
    )
    swap.start()
    swap.wait()
    both = moved[...] + to_slots(theirs, y_recv)
    for h in range(2):
        for part in range(2):
            send1[:, 2 * part + h, :] = both[128 * part : 128 * part + 128, 128 * h : 128 * h + 128]

    def to_all(send, phases):
        for phase in phases:
            slabs = [(way, lax.rem(mesh_z + way, GROUPS)) for way in phase]

            def row(d, skip):
                at = lax.rem(in_z + d, MEMBERS)
                base = MEMBERS * (at // 2) + lax.rem(at, 2)
                for way, there in slabs:
                    if not (skip and way == 0):
                        send(base + 2 * there, MEMBERS * there + at)

            def one(d, carry):
                row(d, False)
                return carry

            row(0, True)
            lax.fori_loop(1, MEMBERS, one, 0)

    def send_ids(peer, at):
        pltpu.make_async_remote_copy(
            send1.at[at], recv1.at[mine_at], a_s, a_r.at[mesh_z], device_id={"tbl": peer}, device_id_type=MESH
        ).start()

    to_all(send_ids, ((1, 7, 0), (2, 6), (3, 5, 4)))
    recv1[mine_at] = send1[mine_at]

    bag = (
        4 * lax.rem(lax.broadcasted_iota(I32, (MEMBERS, 4, 128), 0), 2)
        + lax.broadcasted_iota(I32, (MEMBERS, 4, 128), 2) // 32
    ).astype(F32)
    line = lax.broadcasted_iota(I32, (256, 128), 0).astype(F32).astype(BF16)
    along = lax.broadcasted_iota(I32, (128, 256), 1).astype(F32).astype(BF16)
    unit = identity(128)

    def arrived(n, where):
        return pltpu.make_async_remote_copy(
            send1.at[pl.ds(0, n)], recv1.at[pl.ds(0, n)], a_s, a_r.at[where],
            device_id={"rep": other}, device_id_type=MESH,
        )

    def spread(row):
        x = jnp.broadcast_to(row, (16, 128)).astype(BF16)
        return jnp.concatenate([x] * 16, axis=0)

    def count_group(src):
        base = src * MEMBERS
        ids = recv1[pl.ds(base, MEMBERS)]
        row = ids - jnp.floor((ids + 0.5) * share) * rows
        top = jnp.floor(row * (1.0 / LO))
        key[...] = top * 8.0 + bag
        low = (row - top * LO).reshape(4 * MEMBERS, 128)
        turned[...] = dot_nt(unit, low.astype(BF16))
        for p in range(MEMBERS // 2):
            left, right = [], []
            for h in range(2):
                for i in (2 * p, 2 * p + 1):
                    hit = spread(key[i, pl.ds(h, 1), :]) == line
                    left.append(jnp.where(hit, spread(recv1[base + i, pl.ds(2 + h, 1), :]), jnp.bfloat16(0)))
                    at = 4 * i + h
                    column = jnp.broadcast_to(turned[:, at : at + 1], (128, 256)).astype(BF16)
                    right.append(jnp.where(column == along, jnp.bfloat16(1), jnp.bfloat16(0)))
            total = jnp.dot(
                jnp.concatenate(left, axis=1), jnp.concatenate(right, axis=0), preferred_element_type=F32
            )
            at = pl.multiple_of(4 * MEMBERS * src, 8) + 8 * p
            for c in range(2):
                count[c, :, pl.ds(at, 8), :] = total[:, 128 * c : 128 * c + 128].reshape(HI, 8, 128)

    def count_step(d, carry):
        near = (d + 1) // 2
        src = lax.rem(mesh_z + jnp.where(lax.rem(d, 2) == 1, near, GROUPS - near), GROUPS)
        arrived(MEMBERS, src).wait_recv()
        count_group(src)
        return carry

    arrived(MEMBERS - 1, mesh_z).wait_recv()
    count_group(mesh_z)
    lax.fori_loop(1, GROUPS, count_step, 0)
    load.wait()

    for block in BLOCKS:
        used = pl.ds(0, 256 * len(block))

        def pool(g, carry):
            total = None
            for i in range(STEP):
                hi = STEP * g + i
                stack = []
                for q in block:
                    x = jnp.concatenate([count[c, hi, pl.ds(q, 128, stride=4), :] for c in range(2)], axis=1)
                    stack += split2(x)
                part = jnp.dot(
                    jnp.concatenate(stack, axis=0),
                    table[pl.ds(pl.multiple_of(hi * LO, LO), LO), :],
                    preferred_element_type=F32,
                )
                total = part if total is None else total + part

            @pl.when(g == 0)
            def _():
                acc[used, :] = total

            @pl.when(g > 0)
            def _():
                acc[used, :] += total

            return carry

        lax.fori_loop(0, HI // STEP, pool, 0)
        for ch, (at, size) in enumerate(CHUNKS):
            if at not in block:
                continue
            for q in range(size):
                for c in range(2):
                    cols = pl.ds(128 * c, 128)
                    up = 256 * (at + q - block[0])
                    send2[ch][:, 2 * q + c, :] = acc[pl.ds(up, 128), cols] + acc[pl.ds(up + 128, 128), cols]

            def send_sums(peer, at):
                pltpu.make_async_remote_copy(
                    send2[ch].at[at], recv2[ch].at[me], b_s.at[ch], b_r.at[ch],
                    device_id={"tbl": peer}, device_id_type=MESH,
                ).start()

            to_all(send_sums, ((4, 1, 7, 2, 6, 3, 5, 0),))
            recv2[ch][me] = send2[ch][mine_at]

    arrived(SLOTS - 1, 0).wait_send()
    ends = []
    for ch, (at, size) in enumerate(CHUNKS):
        everyone = pltpu.make_async_remote_copy(
            send2[ch].at[pl.ds(0, SLOTS - 1)], recv2[ch].at[pl.ds(0, SLOTS - 1)], b_s.at[ch], b_r.at[ch],
            device_id={"rep": other}, device_id_type=MESH,
        )
        everyone.wait_recv()

        def give(k, carry):
            p_send[ch][k] = recv2[ch][ts_smem[64 * other + k]]
            return carry

        lax.fori_loop(0, 64, give, 0, unroll=8)
        back = pltpu.make_async_remote_copy(
            p_send[ch], p_recv[ch], c_s.at[ch], c_r.at[ch], device_id={"rep": other}, device_id_type=MESH
        )
        back.start()
        ends.append((everyone, back))

        def keep(k, carry):
            kept[ch][k] = recv2[ch][ts_smem[64 * rep + k]]
            return carry

        lax.fori_loop(0, 64, keep, 0, unroll=8)
        place(out_ref, kept[ch], inverse, rep, at)
    for ch, (at, size) in enumerate(CHUNKS):
        everyone, back = ends[ch]
        back.wait()
        place(out_ref, p_recv[ch], inverse, other, at)
        everyone.wait_send()


def per_device(embeddings, raw_ids, id_weights, lengths, table_slot, table_rows):
    ids = jnp.transpose(raw_ids, (2, 0, 1)).reshape(8 * BAG, 64)
    weights = jnp.transpose(id_weights, (2, 0, 1)).reshape(8 * BAG, 64)
    vmem = pl.BlockSpec(memory_space=pltpu.VMEM)
    dma = pltpu.SemaphoreType.DMA
    return pl.pallas_call(
        kernel,
        out_shape=jax.ShapeDtypeStruct((8, 64, 256), F32),
        in_specs=[pl.BlockSpec(memory_space=pltpu.SMEM)] + [pl.BlockSpec(memory_space=pltpu.HBM)] * 6,
        out_specs=vmem,
        scratch_shapes=[
            pltpu.VMEM((8 * BAG, 64), F32),
            pltpu.VMEM((256, 128), F32),
            pltpu.VMEM((256, 128), F32),
            pltpu.VMEM((256, 128), F32),
            pltpu.VMEM((SLOTS, 4, 128), F32),
            pltpu.VMEM((256, 256), F32),
            pltpu.VMEM((SLOTS, 4, 128), F32),
            pltpu.VMEM((MEMBERS, 4, 128), F32),
            pltpu.VMEM((128, 4 * MEMBERS), F32),
            pltpu.VMEM((8, 64, 128), F32),
            pltpu.VMEM((2, HI, 512, 128), F32),
            pltpu.VMEM((ROWS, 256), BF16),
            pltpu.VMEM((512, 256), F32),
            pltpu.VMEM((1, 128), I32),
            pltpu.VMEM((1, 128), I32),
            pltpu.VMEM((8 * BAG, 64), I32),
            pltpu.VMEM((8 * BAG, 64), BF16),
            pltpu.VMEM((8, 64), I32),
            dma((5,)),
            dma, dma, dma, dma, dma((GROUPS,)),
            dma((len(CHUNKS),)), dma((len(CHUNKS),)), dma((len(CHUNKS),)), dma((len(CHUNKS),)),
        ]
        + [
            pltpu.VMEM((n, 2 * size, 128), F32)
            for _, size in CHUNKS
            for n in (SLOTS, SLOTS, 64, 64, 64)
        ],
        compiler_params=pltpu.CompilerParams(
            collective_id=0, has_side_effects=True, vmem_limit_bytes=61 * 1024 * 1024
        ),
    )(table_slot, table_slot.reshape(1, 128), table_rows.reshape(1, 128), ids, weights, lengths, embeddings)


def solution(mesh):
    in_specs = (
        P("tbl", None),
        P("tbl", "rep", None),
        P("tbl", "rep", None),
        P("tbl", "rep"),
        P(),
        P(),
    )
    return jax.shard_map(
        per_device, mesh=mesh, in_specs=in_specs, out_specs=P("tbl", "rep", None), check_vma=False
    )
```

```python
import functools

import jax
import jax.numpy as jnp
from jax import lax
from jax.experimental import pallas as pl
from jax.experimental.pallas import tpu as pltpu
from jax.sharding import PartitionSpec as P

MESH = pl.DeviceIdType.MESH
F32, BF16, I32 = jnp.float32, jnp.bfloat16, jnp.int32
SLOTS = 128
BAG = 60
ROWS = 8192
LO = 256
HI = ROWS // LO
CHUNKS = ((0, 1), (1, 1), (2, 1), (3, 1))
BLOCKS = ((0,), (1,), (2,), (3,))
MEMBERS = 16
GROUPS = SLOTS // MEMBERS
STEP = 16


def dot_nt(a, b):
    return lax.dot_general(a, b, (((1,), (1,)), ((), ())), preferred_element_type=F32)


def split2(x):
    top = x.astype(BF16)
    return top, (x - top.astype(F32)).astype(BF16)


def build_rows(y_ref, ids_ref, wf_ref, len_ref, half):
    for q in range(4):
        req = 4 * half + q
        count = len_ref[pl.ds(req, 1), :]
        for h in range(2):
            n = 32 if h == 0 else BAG - 32
            start = req + 256 * h
            ids = ids_ref[pl.ds(start, n, stride=8), :].astype(F32)
            w = wf_ref[pl.ds(start, n, stride=8), :]
            pos = lax.broadcasted_iota(I32, (n, 64), 0) + 32 * h
            w = jnp.where(pos < count, w, 0.0)
            y_ref[pl.ds((h * 4 + q) * 32, n), :] = jnp.concatenate([ids, w], axis=1)
            if n < 32:
                y_ref[pl.ds((h * 4 + q) * 32 + n, 32 - n), :] = jnp.zeros((32 - n, 128), F32)


def to_slots(slot_of_lane, y_ref):
    row = lax.broadcasted_iota(I32, (256, 128), 0)
    lane = lax.broadcasted_iota(I32, (256, 128), 1)
    slot = jnp.where(row < 128, row, row - 128)
    pick = (slot_of_lane == slot) & ((row < 128) == (lane < 64))
    pick = jnp.where(pick, 1.0, 0.0).astype(BF16)
    top, rest = split2(y_ref[...])
    return dot_nt(pick, top) + dot_nt(pick, rest)


def place(out_ref, held, inverse, half, first):
    for q in range(held.shape[1] // 2):
        req = 4 * half + first + q
        for c in range(2):
            out_ref[req, :, pl.ds(128 * c, 128)] = held[:, 2 * q + c, :] * inverse[req]


def by_z(slot):
    return MEMBERS * (slot // 2 % GROUPS) + 2 * (slot // MEMBERS) + slot % 2


def identity(n):
    row = lax.broadcasted_iota(I32, (n, n), 0)
    return jnp.where(row == lax.broadcasted_iota(I32, (n, n), 1), 1.0, 0.0).astype(BF16)


def kernel(
    ts_smem, ts_hbm, tr_hbm, ids_hbm, w_hbm, len_hbm, emb_ref,
    out_ref,
    wf, y_own, y_send, y_recv, send1, moved, recv1, key, turned, inverse, count, table, acc,
    ts_ref, tr_ref, ids_ref, w_ref, len_ref, in_sem, emb_sem, rep_s, rep_r, a_s, a_r, b_s, b_r, c_s, c_r,
    *buffers,
):
    send2, recv2, p_send, p_recv, kept = (buffers[i :: 5] for i in range(5))
    me = lax.axis_index("tbl")
    rep = lax.axis_index("rep")
    other = 1 - rep
    mesh_z = lax.rem(me // 2, GROUPS)
    in_z = 2 * (me // MEMBERS) + lax.rem(me, 2)
    mine_at = MEMBERS * mesh_z + in_z

    inputs = [
        pltpu.make_async_copy(src, dst, in_sem.at[i])
        for i, (src, dst) in enumerate(
            [(ids_hbm, ids_ref), (w_hbm, w_ref), (len_hbm, len_ref), (ts_hbm, ts_ref), (tr_hbm, tr_ref)]
        )
    ]
    for copy in inputs:
        copy.start()
    barrier = pltpu.get_barrier_semaphore()

    def greet(d, carry):
        peer = lax.rem(me + d, SLOTS)
        pl.semaphore_signal(barrier, inc=1, device_id={"tbl": peer}, device_id_type=MESH)
        return carry

    lax.fori_loop(1, SLOTS, greet, 0)
    pl.semaphore_signal(barrier, inc=1, device_id={"rep": other}, device_id_type=MESH)

    load = pltpu.make_async_copy(emb_ref, table, emb_sem)
    load.start()

    for copy in inputs:
        copy.wait()
    wf[...] = w_ref[...].astype(F32)
    build_rows(y_send, ids_ref, wf, len_ref, other)
    build_rows(y_own, ids_ref, wf, len_ref, rep)
    lane = lax.broadcasted_iota(I32, (1, 128), 1)
    slots = by_z(ts_ref[...])
    rolled = pltpu.roll(slots, 64, 1)
    first = jnp.where(lane < 64, slots, rolled)
    second = jnp.where(lane < 64, rolled, slots)
    mine = jnp.where(rep == 0, first, second)
    theirs = jnp.where(rep == 0, second, first)
    moved[...] = to_slots(mine, y_own)
    columns = 1.0 / dot_nt(identity(64), len_ref[...].astype(F32).astype(BF16))
    for req in range(8):
        inverse[req] = jnp.broadcast_to(columns[:, req : req + 1], (64, 128))
    rows = jnp.sum(jnp.where(slots == mine_at, tr_ref[...], 0), axis=1, keepdims=True).astype(F32)
    share = 1.0 / rows

    pl.semaphore_wait(barrier, SLOTS)
    swap = pltpu.make_async_remote_copy(
        y_send, y_recv, rep_s, rep_r, device_id={"rep": other}, device_id_type=MESH
    )
    swap.start()
    swap.wait()
    both = moved[...] + to_slots(theirs, y_recv)
    for h in range(2):
        for part in range(2):
            send1[:, 2 * part + h, :] = both[128 * part : 128 * part + 128, 128 * h : 128 * h + 128]

    def to_all(send, phases):
        for phase in phases:
            slabs = [(way, lax.rem(mesh_z + way, GROUPS)) for way in phase]

            def row(d, skip):
                at = lax.rem(in_z + d, MEMBERS)
                base = MEMBERS * (at // 2) + lax.rem(at, 2)
                for way, there in slabs:
                    if not (skip and way == 0):
                        send(base + 2 * there, MEMBERS * there + at)

            def one(d, carry):
                row(d, False)
                return carry

            row(0, True)
            lax.fori_loop(1, MEMBERS, one, 0)

    def send_ids(peer, at):
        pltpu.make_async_remote_copy(
            send1.at[at], recv1.at[mine_at], a_s, a_r.at[mesh_z], device_id={"tbl": peer}, device_id_type=MESH
        ).start()

    to_all(send_ids, ((0,), (1, 7), (2, 6), (3, 5), (4,)))
    recv1[mine_at] = send1[mine_at]

    bag = (
        4 * lax.rem(lax.broadcasted_iota(I32, (MEMBERS, 4, 128), 0), 2)
        + lax.broadcasted_iota(I32, (MEMBERS, 4, 128), 2) // 32
    ).astype(F32)
    line = lax.broadcasted_iota(I32, (256, 128), 0).astype(F32).astype(BF16)
    along = lax.broadcasted_iota(I32, (128, 256), 1).astype(F32).astype(BF16)
    unit = identity(128)

    def arrived(n, where):
        return pltpu.make_async_remote_copy(
            send1.at[pl.ds(0, n)], recv1.at[pl.ds(0, n)], a_s, a_r.at[where],
            device_id={"rep": other}, device_id_type=MESH,
        )

    def spread(row):
        x = jnp.broadcast_to(row, (16, 128)).astype(BF16)
        return jnp.concatenate([x] * 16, axis=0)

    def count_group(src):
        base = src * MEMBERS
        ids = recv1[pl.ds(base, MEMBERS)]
        row = ids - jnp.floor((ids + 0.5) * share) * rows
        top = jnp.floor(row * (1.0 / LO))
        key[...] = top * 8.0 + bag
        low = (row - top * LO).reshape(4 * MEMBERS, 128)
        turned[...] = dot_nt(unit, low.astype(BF16))
        for p in range(MEMBERS // 2):
            left, right = [], []
            for h in range(2):
                for i in (2 * p, 2 * p + 1):
                    hit = spread(key[i, pl.ds(h, 1), :]) == line
                    left.append(jnp.where(hit, spread(recv1[base + i, pl.ds(2 + h, 1), :]), jnp.bfloat16(0)))
                    at = 4 * i + h
                    column = jnp.broadcast_to(turned[:, at : at + 1], (128, 256)).astype(BF16)
                    right.append(jnp.where(column == along, jnp.bfloat16(1), jnp.bfloat16(0)))
            total = jnp.dot(
                jnp.concatenate(left, axis=1), jnp.concatenate(right, axis=0), preferred_element_type=F32
            )
            at = pl.multiple_of(4 * MEMBERS * src, 8) + 8 * p
            for c in range(2):
                count[c, :, pl.ds(at, 8), :] = total[:, 128 * c : 128 * c + 128].reshape(HI, 8, 128)

    def count_step(d, carry):
        near = (d + 1) // 2
        src = lax.rem(mesh_z + jnp.where(lax.rem(d, 2) == 1, near, GROUPS - near), GROUPS)
        arrived(MEMBERS, src).wait_recv()
        count_group(src)
        return carry

    arrived(MEMBERS - 1, mesh_z).wait_recv()
    count_group(mesh_z)
    lax.fori_loop(1, GROUPS, count_step, 0)
    load.wait()

    for block in BLOCKS:
        used = pl.ds(0, 256 * len(block))

        def pool(g, carry):
            total = None
            for i in range(STEP):
                hi = STEP * g + i
                stack = []
                for q in block:
                    x = jnp.concatenate([count[c, hi, pl.ds(q, 128, stride=4), :] for c in range(2)], axis=1)
                    stack += split2(x)
                part = jnp.dot(
                    jnp.concatenate(stack, axis=0),
                    table[pl.ds(pl.multiple_of(hi * LO, LO), LO), :],
                    preferred_element_type=F32,
                )
                total = part if total is None else total + part

            @pl.when(g == 0)
            def _():
                acc[used, :] = total

            @pl.when(g > 0)
            def _():
                acc[used, :] += total

            return carry

        lax.fori_loop(0, HI // STEP, pool, 0)
        for ch, (at, size) in enumerate(CHUNKS):
            if at not in block:
                continue
            for q in range(size):
                for c in range(2):
                    cols = pl.ds(128 * c, 128)
                    up = 256 * (at + q - block[0])
                    send2[ch][:, 2 * q + c, :] = acc[pl.ds(up, 128), cols] + acc[pl.ds(up + 128, 128), cols]

            def send_sums(peer, at):
                pltpu.make_async_remote_copy(
                    send2[ch].at[at], recv2[ch].at[me], b_s.at[ch], b_r.at[ch],
                    device_id={"tbl": peer}, device_id_type=MESH,
                ).start()

            to_all(send_sums, ((4, 1, 7, 2, 6, 3, 5, 0),))
            recv2[ch][me] = send2[ch][mine_at]

    arrived(SLOTS - 1, 0).wait_send()
    ends = []
    for ch, (at, size) in enumerate(CHUNKS):
        everyone = pltpu.make_async_remote_copy(
            send2[ch].at[pl.ds(0, SLOTS - 1)], recv2[ch].at[pl.ds(0, SLOTS - 1)], b_s.at[ch], b_r.at[ch],
            device_id={"rep": other}, device_id_type=MESH,
        )
        everyone.wait_recv()

        def give(k, carry):
            p_send[ch][k] = recv2[ch][ts_smem[64 * other + k]]
            return carry

        lax.fori_loop(0, 64, give, 0, unroll=8)
        back = pltpu.make_async_remote_copy(
            p_send[ch], p_recv[ch], c_s.at[ch], c_r.at[ch], device_id={"rep": other}, device_id_type=MESH
        )
        back.start()
        ends.append((everyone, back))

        def keep(k, carry):
            kept[ch][k] = recv2[ch][ts_smem[64 * rep + k]]
            return carry

        lax.fori_loop(0, 64, keep, 0, unroll=8)
        place(out_ref, kept[ch], inverse, rep, at)
    for ch, (at, size) in enumerate(CHUNKS):
        everyone, back = ends[ch]
        back.wait()
        place(out_ref, p_recv[ch], inverse, other, at)
        everyone.wait_send()


def per_device(embeddings, raw_ids, id_weights, lengths, table_slot, table_rows):
    ids = jnp.transpose(raw_ids, (2, 0, 1)).reshape(8 * BAG, 64)
    weights = jnp.transpose(id_weights, (2, 0, 1)).reshape(8 * BAG, 64)
    vmem = pl.BlockSpec(memory_space=pltpu.VMEM)
    dma = pltpu.SemaphoreType.DMA
    return pl.pallas_call(
        kernel,
        out_shape=jax.ShapeDtypeStruct((8, 64, 256), F32),
        in_specs=[pl.BlockSpec(memory_space=pltpu.SMEM)] + [pl.BlockSpec(memory_space=pltpu.HBM)] * 6,
        out_specs=vmem,
        scratch_shapes=[
            pltpu.VMEM((8 * BAG, 64), F32),
            pltpu.VMEM((256, 128), F32),
            pltpu.VMEM((256, 128), F32),
            pltpu.VMEM((256, 128), F32),
            pltpu.VMEM((SLOTS, 4, 128), F32),
            pltpu.VMEM((256, 256), F32),
            pltpu.VMEM((SLOTS, 4, 128), F32),
            pltpu.VMEM((MEMBERS, 4, 128), F32),
            pltpu.VMEM((128, 4 * MEMBERS), F32),
            pltpu.VMEM((8, 64, 128), F32),
            pltpu.VMEM((2, HI, 512, 128), F32),
            pltpu.VMEM((ROWS, 256), BF16),
            pltpu.VMEM((512, 256), F32),
            pltpu.VMEM((1, 128), I32),
            pltpu.VMEM((1, 128), I32),
            pltpu.VMEM((8 * BAG, 64), I32),
            pltpu.VMEM((8 * BAG, 64), BF16),
            pltpu.VMEM((8, 64), I32),
            dma((5,)),
            dma, dma, dma, dma, dma((GROUPS,)),
            dma((len(CHUNKS),)), dma((len(CHUNKS),)), dma((len(CHUNKS),)), dma((len(CHUNKS),)),
        ]
        + [
            pltpu.VMEM((n, 2 * size, 128), F32)
            for _, size in CHUNKS
            for n in (SLOTS, SLOTS, 64, 64, 64)
        ],
        compiler_params=pltpu.CompilerParams(
            collective_id=0, has_side_effects=True, vmem_limit_bytes=61 * 1024 * 1024
        ),
    )(table_slot, table_slot.reshape(1, 128), table_rows.reshape(1, 128), ids, weights, lengths, embeddings)


def solution(mesh):
    in_specs = (
        P("tbl", None),
        P("tbl", "rep", None),
        P("tbl", "rep", None),
        P("tbl", "rep"),
        P(),
        P(),
    )
    return jax.shard_map(
        per_device, mesh=mesh, in_specs=in_specs, out_specs=P("tbl", "rep", None), check_vma=False
    )
```
